32 devices in a mesh: row: 4 (over y, x), col: 8 (over z, core).
Axes of the slice: x: 2, y: 2, z: 4, core: 2. Of those that a mesh axis runs over, the one named last changes fastest.
Arguments:
- residuals: bfloat16 [32768, 768], P(('row', 'col')), may hold values from -6 to 6
- codes: int32 [32768, 64], P(('row', 'col')), may hold values from 0 to 255
- list_ids: int32 [32768], P(('row', 'col')), may hold values from 0 to 8191, as said below
- rotation: bfloat16 [768, 768], replicated, may hold values from -0.21875 to 0.21875
- codebook: bfloat16 [256, 768], replicated, may hold values from -6 to 6
- list_fill: int32 [8192], P(('row', 'col')), may hold values from 0 to 4095
Outputs:
- list_drift: float32 [8192, 768], P(('row', 'col'))
- list_counts: int32 [8192], P(('row', 'col'))
- new_blocks: int32 [8192], P(('row', 'col'))
The draws below stay inside these ranges and needn't reach their ends.
Inputs may be any that keep to these rules, and one draw needn't show every extreme that they name: `list_ids`: lists are grouped in blocks of 256 consecutive ids. Among the rows of one device (aligned blocks of 1024 rows), at most 96 have lists in the same block, and in every such aligned block some list block is named by exactly 96 rows.
All inputs are finite; a program needn't handle non-finite values.
Results may differ from the reference program's by a relative error of at most 0.0029.
Values may be sent and summed in bfloat16 or wider, within the bound.
No kernel may reach another device: no remote copies, remote signals or barrier semaphores. Data moves between devices by JAX's collectives and lax.ppermute only.
A program may use at most 64 MiB of HBM per device.

```python
import jax
import jax.numpy as jnp
from jax import lax

D = 768
M = 64
KSUB = 256
LISTS_DEV = 256
VEC_DEV = 1024
DSUB = 12
OWNERS = 32
LISTS = 8192
NVEC = 32768
SLOTS = 96


def device_plan(device_key):
    key_hot, key_spread, key_inner, key_order = jax.random.split(device_key, 4)
    hot_owner = jax.random.randint(key_hot, (), 0, OWNERS)
    positions = jax.random.permutation(key_spread, (OWNERS - 1) * SLOTS)[:VEC_DEV - SLOTS]
    others = positions // SLOTS
    others = others + (others >= hot_owner).astype(jnp.int32)
    owner_of = jnp.concatenate([jnp.full((SLOTS,), hot_owner, jnp.int32), others.astype(jnp.int32)])
    inner = jax.random.randint(key_inner, (VEC_DEV,), 0, LISTS_DEV)
    order = jax.random.permutation(key_order, VEC_DEV)
    ids = owner_of * LISTS_DEV + inner
    return ids[order]


def draw_list_ids(key, part):
    base = jax.random.fold_in(key, 7)
    device_keys = jax.vmap(lambda index: jax.random.fold_in(base, index))(jnp.arange(OWNERS))
    return jax.vmap(device_plan)(device_keys).reshape(-1)


def plant(drawn, rng, smallest, high):
    shape = drawn.shape
    index_at = [jax.random.randint(jax.random.fold_in(rng, axis), (), 0, shape[axis]) for axis in range(len(shape))]
    drawn = drawn.at[tuple(index_at)].set(smallest)
    longest = shape.index(max(shape))
    index_at[longest] = (index_at[longest] + 1) % shape[longest]
    return drawn.at[tuple(index_at)].set(high)


def block_levels(stream_key, shape, cuts, low, top_value):
    loudness, own = 1.0, jax.random.fold_in(stream_key, 6)
    for dim, parts in cuts:
        heights = jnp.exp(jax.random.uniform(jax.random.fold_in(own, dim), (parts,), jnp.float32, low / len(cuts), top_value / len(cuts)))
        loudness = loudness * jnp.repeat(heights, shape[dim] // parts).reshape([-1 if axis == dim else 1 for axis in range(len(shape))])
    return loudness


def normal_values(own_key, dims, scale, most, cuts=(), held_as=jnp.bfloat16):
    result = jax.random.normal(own_key, dims, jnp.float32) * scale
    if len(cuts) > 0:
        result = block_levels(own_key, dims, cuts, -0.22, 0.18) * result
    return jnp.clip(result, min=-most, max=most).astype(held_as)


def setup_inputs(seed: int = 0) -> dict:
    splits = jax.random.split(jax.random.key(seed), 7)
    residuals = normal_values(splits[0], (NVEC, D), 1.0, 6.0, ((0, 32),))
    codes = plant(jax.random.randint(splits[1], (NVEC, M), 0, KSUB), jax.random.fold_in(splits[1], 1), 0, KSUB - 1).astype(jnp.int32)
    list_ids = draw_list_ids(jax.random.fold_in(splits[6], 71), 0)
    rotation = normal_values(splits[3], (D, D), D ** -0.5, 0.21875)
    codebook = normal_values(splits[4], (KSUB, D), 1.0, 6.0)
    list_fill = plant(jax.random.randint(splits[5], (LISTS,), 0, 4096), jax.random.fold_in(splits[5], 1), 0, 4095).astype(jnp.int32)
    return {"residuals": residuals, "codes": codes, "list_ids": list_ids, "rotation": rotation, "codebook": codebook, "list_fill": list_fill}


def reference(residuals, codes, list_ids, rotation, codebook, list_fill):
    block_rows = VEC_DEV * 8
    turns = NVEC // block_rows
    code_table = codebook.reshape(KSUB, M, DSUB)
    sub_index = jnp.arange(M, dtype=jnp.int32)

    def step(carry, pieces):
        list_sums, counts = carry
        res_block, code_block, id_block = pieces
        rotated = jnp.dot(res_block, rotation, preferred_element_type=jnp.float32)
        rebuilt = code_table[code_block, sub_index[None, :], :].astype(jnp.float32).reshape(block_rows, D)
        encode_error = (rotated - rebuilt).astype(jnp.bfloat16)
        list_sums = list_sums + jax.ops.segment_sum(encode_error.astype(jnp.float32), id_block, num_segments=LISTS)
        counts = counts + jax.ops.segment_sum(jnp.ones((block_rows,), jnp.int32), id_block, num_segments=LISTS)
        return (list_sums, counts), None

    start = (jnp.zeros((LISTS, D), jnp.float32), jnp.zeros((LISTS,), jnp.int32))
    pieces = (residuals.reshape(turns, block_rows, D), codes.reshape(turns, block_rows, M), list_ids.reshape(turns, block_rows))
    (list_sums, list_counts), _ = lax.scan(step, start, pieces)
    divisor = jnp.maximum(list_counts, 1).astype(jnp.float32)
    list_drift = list_sums / divisor[:, None]
    new_blocks = (list_fill + list_counts + 127) // 128 - (list_fill + 127) // 128
    return list_drift, list_counts, new_blocks
```

```python
import functools

import jax
import jax.numpy as jnp
from jax import lax
from jax.experimental import pallas as pl
from jax.experimental.pallas import tpu as pltpu
from jax.sharding import PartitionSpec as P

CHUNKS = 3
F32 = jnp.float32
BF16 = jnp.bfloat16
NT = (((1,), (1,)), ((), ()))


def up(value, step):
    return (value + step - 1) // step * step


def tag_rows(slots, width):
    return up(8 * (-(-slots // width)), 16)


def iota(shape, dim):
    return lax.broadcasted_iota(jnp.int32, shape, dim)


def hot(test):
    return jnp.where(test, 1.0, 0.0).astype(F32)


def split(total, pieces):
    while total % (128 * pieces):
        pieces -= 1
    return total // pieces


def plan_slots(ids, slots, lists_here, row_count, col_count):
    me = lax.axis_index("row")
    vecs = ids.shape[1]
    owner = ids // lists_here
    group = (owner // col_count) ^ me
    owner_col = owner % col_count
    in_list = ids % lists_here
    sub = max(8, row_count)
    member = hot(iota((sub, vecs), 0) == group)
    run = member
    lane = iota((sub, vecs), 1)
    step = 1
    while step < vecs:
        run = run + jnp.where(lane >= step, pltpu.roll(run, step, 1), 0.0)
        step *= 2
    rank = jnp.sum((run - member) * member, axis=0, keepdims=True).astype(jnp.int32)
    slot = jnp.where(rank < slots, group * slots + rank, -1)
    tags = jnp.where(
        iota((16, vecs), 0) == 0,
        (owner_col + 1).astype(F32),
        jnp.where(iota((16, vecs), 0) == 1, in_list.astype(F32), 0.0),
    )
    return slot, tags.astype(BF16)


def pack_kernel(first, slots, base, width, dsub, lists_here, row_count, col_count, *refs):
    if first:
        ids_ref, codes_ref, res_ref, rot_ref, book_ref = refs[:5]
        outs = refs[5 : 5 + row_count]
        slot_ref, ct_ref, rot_t, tab_t, err_t = refs[5 + row_count :]
        ct_ref[...] = codes_ref[...].T
        slot, tags = plan_slots(ids_ref[...], slots, lists_here, row_count, col_count)
        slot_ref[...] = jnp.broadcast_to(slot, slot_ref.shape)
    else:
        slot_ref, ct_ref, res_ref, rot_ref, book_ref = refs[:5]
        outs = refs[5 : 5 + row_count]
        rot_t, tab_t, err_t = refs[5 + row_count :]
        slot = slot_ref[0:1, :]
    vecs = res_ref.shape[0]
    cents = book_ref.shape[0]
    tab_t[...] = book_ref[...].astype(F32).T
    rot_t[...] = lax.dot_general(
        rot_ref[...], res_ref[...], (((0,), (1,)), ((), ())), preferred_element_type=F32
    )

    def lanes(block, carry):
        here = pl.ds(pl.multiple_of(block * 128, 128), 128)

        def half(row):
            first_sub = (base + row) // dsub
            last_sub = (base + row + 7) // dsub
            index = jnp.broadcast_to(ct_ref[first_sub : first_sub + 1, here], (8, 128))
            for sub in range(first_sub + 1, last_sub + 1):
                starts = sub * dsub - (base + row)
                other = jnp.broadcast_to(ct_ref[sub : sub + 1, here], (8, 128))
                index = jnp.where(iota((8, 128), 0) >= starts, other, index)
            low = index & 127
            value = None
            for part in range(0, cents, 128):
                got = jnp.take_along_axis(
                    tab_t[row : row + 8, part : part + 128], low, axis=1, mode="promise_in_bounds"
                )
                value = got if value is None else jnp.where(index >= part, got, value)
            return rot_t[row : row + 8, here] - value

        for row in range(0, width, 16):
            err_t[row : row + 16, here] = jnp.concatenate([half(row), half(row + 8)], 0).astype(BF16)
        return carry

    lax.fori_loop(0, vecs // 128, lanes, 0)
    err = err_t[...]
    for group in range(row_count):
        picker = hot(iota((slots, vecs), 0) + group * slots == slot).astype(BF16)
        rows = lax.dot_general(picker, err, NT, preferred_element_type=F32)
        outs[group][0:slots, :] = rows.astype(BF16)
        if first:
            line = lax.dot_general(tags, picker, NT, preferred_element_type=F32)[0:8, :]
            extra = outs[group].shape[0] - slots
            parts = [line[:, at : min(at + width, slots)] for at in range(0, slots, width)]
            parts = [
                part
                if part.shape[1] == width
                else jnp.concatenate([part, jnp.zeros((8, width - part.shape[1]), F32)], 1)
                for part in parts
            ]
            while len(parts) * 8 < extra:
                parts.append(jnp.zeros((8, width), F32))
            outs[group][slots:, :] = jnp.concatenate(parts, 0).astype(BF16)


def sum_kernel(first, slots, width, lists_here, row_count, zone_count, *refs):
    senders = 2 * row_count
    lane_count = senders * slots
    if first:
        got = refs[:senders]
        blocks = refs[senders : senders + zone_count]
        count_ref, key_ref, rows = refs[senders + zone_count :]
        me = lax.axis_index("col")
        zone, core = me // 2, me % 2
        keys = []
        for ref in got:
            extra = ref[slots:, :].astype(F32)
            pieces = -(-slots // width)
            line = jnp.concatenate([extra[8 * p : 8 * p + 8, :] for p in range(pieces)], 1)
            line = line[:, 0:slots].astype(jnp.int32)
            owner_col = line[0:1, :] - 1
            key = ((owner_col >> 1) ^ zone) * lists_here + line[1:2, :]
            mine = (owner_col >= 0) & ((owner_col & 1) == core)
            keys.append(jnp.where(mine, key, -1))
        for b in range(senders):
            key_ref[b : b + 1, :] = keys[b]
    else:
        key_ref = refs[0]
        got = refs[1 : 1 + senders]
        blocks = refs[1 + senders : 1 + senders + zone_count]
        rows = refs[1 + senders + zone_count]
        keys = [key_ref[b : b + 1, :] for b in range(senders)]
    for b in range(senders):
        rows[b * slots : (b + 1) * slots, :] = got[b][0:slots, :]
    whole = slots % 128 == 0
    if whole:
        keys = [jnp.concatenate(keys, 1)]
    span = lane_count if whole else slots
    for zone_at in range(zone_count):
        total = count = None
        for b, key in enumerate(keys):
            picker = hot(iota((lists_here, span), 0) + zone_at * lists_here == key)
            part = jnp.dot(
                picker.astype(BF16), rows[b * span : (b + 1) * span, :], preferred_element_type=F32
            )
            total = part if total is None else total + part
            if first:
                part = jnp.sum(picker, axis=1, keepdims=True)
                count = part if count is None else count + part
        if zone_at == 0:
            blocks[0][...] = total
        else:
            blocks[zone_at][0:lists_here, :] = total.astype(BF16)
        if first:
            eye = iota((lists_here, lists_here), 0) == iota((lists_here, lists_here), 1)
            line = jnp.sum(jnp.where(eye, count, 0.0), axis=0, keepdims=True)
            if zone_at == 0:
                count_ref[...] = jnp.broadcast_to(line, count_ref.shape)
            else:
                number = line.astype(jnp.int32)
                high = (number >> 8).astype(F32)
                low = (number & 255).astype(F32)
                shape = (16, lists_here)
                extra = jnp.where(
                    iota(shape, 0) == 0, high, jnp.where(iota(shape, 0) == 1, low, 0.0)
                )
                if width > lists_here:
                    extra = jnp.concatenate([extra, jnp.zeros((16, width - lists_here), F32)], 1)
                blocks[zone_at][lists_here:, :] = extra.astype(BF16)


def close_kernel(lists_here, width, chunks, zone_count, *refs):
    fill_ref, own_count = refs[:2]
    refs = refs[2:]
    drift_ref, count_ref, new_ref = refs[chunks * zone_count :]
    line = own_count[0:1, :]
    for at in range(1, zone_count):
        extra = refs[at][lists_here : lists_here + 16, 0:lists_here].astype(F32)
        line = line + extra[0:1, :] * 256.0 + extra[1:2, :]
    number = line.astype(jnp.int32)
    fill = fill_ref[...]
    count_ref[...] = number
    new_ref[...] = ((fill + number + 127) >> 7) - ((fill + 127) >> 7)
    eye = iota((lists_here, lists_here), 0) == iota((lists_here, lists_here), 1)
    divisor = jnp.sum(jnp.where(eye, jnp.maximum(line, 1.0), 0.0), axis=1, keepdims=True)
    for chunk in range(chunks):
        mine = refs[chunk * zone_count : (chunk + 1) * zone_count]
        total = mine[0][...]
        for at in range(1, zone_count):
            total = total + mine[at][0:lists_here, :].astype(F32)
        drift_ref[:, chunk * width : (chunk + 1) * width] = total / divisor


def vmem(count):
    return [pl.BlockSpec(memory_space=pltpu.VMEM)] * count


def call(kernel, outs, scratch, ins, name, flops, specs=None):
    size = sum(a.size * a.dtype.itemsize for a in (*ins, *outs))
    return pl.pallas_call(
        kernel,
        out_shape=outs,
        in_specs=specs or vmem(len(ins)),
        out_specs=vmem(len(outs)),
        scratch_shapes=scratch,
        grid=() if specs is None else (1,),
        name=name,
        cost_estimate=pl.CostEstimate(flops=flops, bytes_accessed=size, transcendentals=0),
        compiler_params=pltpu.CompilerParams(vmem_limit_bytes=56 * 1024 * 1024),
    )(*ins)


def shape(dims, kind):
    return jax.ShapeDtypeStruct(dims, kind)


def local(residuals, codes, list_ids, rotation, codebook, list_fill):
    row_count = lax.axis_size("row")
    col_count = lax.axis_size("col")
    vecs, feats = residuals.shape
    subs = codes.shape[1]
    dsub = feats // subs
    cents = codebook.shape[0]
    lists_here = list_fill.shape[0]
    zone_count = col_count // 2
    width = split(feats, CHUNKS)
    chunks = feats // width
    slots = 3 * vecs // row_count

    def trade(array, axis, size, mask):
        return lax.ppermute(array, axis, [(i, i ^ mask) for i in range(size)])

    ids = list_ids.reshape(1, vecs)
    fill = list_fill.reshape(1, lists_here)
    extra = tag_rows(slots, width)
    packed = []
    slot = codes_t = None
    for chunk in range(chunks):
        first = chunk == 0
        outs = [shape((slots + (extra if first else 0), width), BF16) for _ in range(row_count)]
        scratch = [
            pltpu.VMEM((width, vecs), F32),
            pltpu.VMEM((width, cents), F32),
            pltpu.VMEM((width, vecs), BF16),
        ]
        if first:
            outs += [shape((8, vecs), jnp.int32), shape((subs, vecs), jnp.int32)]
            lead = (ids, codes)
        else:
            lead = (slot, codes_t)
        ins = (*lead, residuals, rotation, codebook)

        def all_of(array):
            return pl.BlockSpec(array.shape, lambda i: (0, 0))

        def columns(array, chunk=chunk):
            return pl.BlockSpec((array.shape[0], width), lambda i: (0, chunk))

        specs = [*map(all_of, ins[:3]), columns(rotation), columns(codebook)]
        got = call(
            functools.partial(
                pack_kernel, first, slots, chunk * width, width, dsub, lists_here, row_count, col_count
            ),
            outs,
            scratch,
            ins,
            f"pack{chunk}",
            2 * vecs * width * (feats + row_count * slots),
            specs,
        )
        packed.append(got[:row_count])
        if first:
            slot, codes_t = got[row_count:]
    blocks = []
    key = count = None
    for chunk in range(chunks):
        first = chunk == 0
        mine = packed[chunk]
        got = [mine[0]] + [None] * (row_count - 1)
        for mask in sorted(range(1, row_count), key=lambda m: -bin(m).count("1")):
            got[mask] = trade(mine[mask], "row", row_count, mask)
        other = [trade(array, "col", col_count, 1) for array in got]
        outs = [shape((lists_here, width), F32)]
        outs += [
            shape((lists_here + (16 if first else 0), width), BF16) for _ in range(zone_count - 1)
        ]
        ins = [*got, *other]
        if first:
            outs += [shape((8, lists_here), F32), shape((2 * row_count, slots), jnp.int32)]
        else:
            ins = [key, *ins]
        sums = call(
            functools.partial(sum_kernel, first, slots, width, lists_here, row_count, zone_count),
            outs,
            [pltpu.VMEM((2 * row_count * slots, width), BF16)],
            ins,
            f"sum{chunk}",
            2 * zone_count * lists_here * 2 * row_count * slots * width,
        )
        if first:
            count, key = sums[zone_count:]
        blocks.append(sums[:zone_count])
    landed = []
    for chunk in range(chunks):
        mine = blocks[chunk]
        landed.append(mine[0])
        got = [None] * zone_count
        for mask in sorted(range(1, zone_count), key=lambda m: -m):
            got[mask] = trade(mine[mask], "col", col_count, 2 * mask)
        landed += got[1:]
    drift, counts, new_blocks = call(
        functools.partial(close_kernel, lists_here, width, chunks, zone_count),
        [
            shape((lists_here, feats), F32),
            shape((1, lists_here), jnp.int32),
            shape((1, lists_here), jnp.int32),
        ],
        [],
        [fill, count, *landed],
        "close",
        lists_here * feats * zone_count,
    )
    return drift, counts.reshape(-1), new_blocks.reshape(-1)


def solution(mesh):
    placed = (
        P(("row", "col"), None),
        P(("row", "col"), None),
        P(("row", "col")),
        P(),
        P(),
        P(("row", "col")),
    )
    return jax.shard_map(
        local,
        mesh=mesh,
        in_specs=placed,
        out_specs=(P(("row", "col"), None), P(("row", "col")), P(("row", "col"))),
        check_vma=False,
    )
```

```python
import functools

import jax
import jax.numpy as jnp
from jax import lax
from jax.experimental import pallas as pl
from jax.experimental.pallas import tpu as pltpu
from jax.sharding import PartitionSpec as P


CHUNKS = 3
F32 = jnp.float32
BF16 = jnp.bfloat16
NT = (((1,), (1,)), ((), ()))


def up(value, step):
    return (value + step - 1) // step * step


def tag_rows(slots, width):
    return up(8 * (-(-slots // width)), 16)


def iota(shape, dim):
    return lax.broadcasted_iota(jnp.int32, shape, dim)


def hot(test):
    return jnp.where(test, 1.0, 0.0).astype(F32)


def split(total, pieces):
    while total % (128 * pieces):
        pieces -= 1
    return total // pieces


def plan_slots(ids, slots, lists_here, row_count, col_count):
    me = lax.axis_index("row")
    vecs = ids.shape[1]
    owner = ids // lists_here
    group = (owner // col_count) ^ me
    owner_col = owner % col_count
    in_list = ids % lists_here
    sub = max(8, row_count)
    member = hot(iota((sub, vecs), 0) == group)
    run = member
    lane = iota((sub, vecs), 1)
    step = 1
    while step < vecs:
        run = run + jnp.where(lane >= step, pltpu.roll(run, step, 1), 0.0)
        step *= 2
    over = jnp.max(hot(run > float(slots)), axis=1, keepdims=True)
    over = jnp.max(over, axis=0, keepdims=True)
    rank = jnp.sum((run - member) * member, axis=0, keepdims=True).astype(jnp.int32)
    slot = jnp.where(rank < slots, group * slots + rank, -1)
    tags = jnp.where(
        iota((16, vecs), 0) == 0,
        (owner_col + 1).astype(F32),
        jnp.where(iota((16, vecs), 0) == 1, in_list.astype(F32), 0.0),
    )
    return slot, tags.astype(BF16), over


def pack_kernel(first, slots, base, width, dsub, lists_here, row_count, col_count, *refs):
    if first:
        ids_ref, ct_ref, res_ref, rot_ref, book_ref = refs[:5]
        outs = refs[5 : 5 + row_count]
        slot_ref, rot_t, tab_t, err_t = refs[5 + row_count :]
        slot, tags, over = plan_slots(ids_ref[...], slots, lists_here, row_count, col_count)
        slot_ref[...] = jnp.broadcast_to(slot, slot_ref.shape)
    else:
        slot_ref, ct_ref, res_ref, rot_ref, book_ref = refs[:5]
        outs = refs[5 : 5 + row_count]
        rot_t, tab_t, err_t = refs[5 + row_count :]
        slot = slot_ref[0:1, :]
    vecs = res_ref.shape[0]
    cents = book_ref.shape[0]
    tab_t[...] = book_ref[...].astype(F32).T
    rot_t[...] = lax.dot_general(
        rot_ref[...], res_ref[...], (((0,), (1,)), ((), ())), preferred_element_type=F32
    )

    def lanes(block, carry):
        here = pl.ds(pl.multiple_of(block * 128, 128), 128)

        def half(row):
            first_sub = (base + row) // dsub
            last_sub = (base + row + 7) // dsub
            index = jnp.broadcast_to(ct_ref[first_sub : first_sub + 1, here], (8, 128))
            for sub in range(first_sub + 1, last_sub + 1):
                starts = sub * dsub - (base + row)
                other = jnp.broadcast_to(ct_ref[sub : sub + 1, here], (8, 128))
                index = jnp.where(iota((8, 128), 0) >= starts, other, index)
            low = index & 127
            value = None
            for part in range(0, cents, 128):
                got = jnp.take_along_axis(
                    tab_t[row : row + 8, part : part + 128], low, axis=1, mode="promise_in_bounds"
                )
                value = got if value is None else jnp.where(index >= part, got, value)
            return rot_t[row : row + 8, here] - value

        for row in range(0, width, 16):
            err_t[row : row + 16, here] = jnp.concatenate([half(row), half(row + 8)], 0).astype(BF16)
        return carry

    lax.fori_loop(0, vecs // 128, lanes, 0)
    err = err_t[...]
    for group in range(row_count):
        picker = hot(iota((slots, vecs), 0) + group * slots == slot).astype(BF16)
        rows = lax.dot_general(picker, err, NT, preferred_element_type=F32)
        outs[group][0:slots, :] = rows.astype(BF16)
        if first:
            line = lax.dot_general(tags, picker, NT, preferred_element_type=F32)[0:8, :]
            line = jnp.where(iota(line.shape, 0) == 2, over, line)
            extra = outs[group].shape[0] - slots
            parts = [line[:, at : min(at + width, slots)] for at in range(0, slots, width)]
            parts = [
                part
                if part.shape[1] == width
                else jnp.concatenate([part, jnp.zeros((8, width - part.shape[1]), F32)], 1)
                for part in parts
            ]
            while len(parts) * 8 < extra:
                parts.append(jnp.zeros((8, width), F32))
            outs[group][slots:, :] = jnp.concatenate(parts, 0).astype(BF16)


def sum_kernel(first, slots, width, lists_here, row_count, zone_count, *refs):
    senders = 2 * row_count
    lane_count = senders * slots
    if first:
        got = refs[:senders]
        blocks = refs[senders : senders + zone_count]
        count_ref, key_ref, rows = refs[senders + zone_count :]
        me = lax.axis_index("col")
        zone, core = me // 2, me % 2
        keys = []
        over = jnp.zeros((1, 1), F32)
        for ref in got:
            extra = ref[slots:, :].astype(F32)
            pieces = -(-slots // width)
            over = over + extra[2:3, 0:1]
            line = jnp.concatenate([extra[8 * p : 8 * p + 8, :] for p in range(pieces)], 1)
            line = line[:, 0:slots].astype(jnp.int32)
            owner_col = line[0:1, :] - 1
            key = ((owner_col >> 1) ^ zone) * lists_here + line[1:2, :]
            mine = (owner_col >= 0) & ((owner_col & 1) == core)
            keys.append(jnp.where(mine, key, -1))
        for b in range(senders):
            key_ref[b : b + 1, :] = keys[b]
    else:
        key_ref = refs[0]
        got = refs[1 : 1 + senders]
        blocks = refs[1 + senders : 1 + senders + zone_count]
        rows = refs[1 + senders + zone_count]
        keys = [key_ref[b : b + 1, :] for b in range(senders)]
    for b in range(senders):
        rows[b * slots : (b + 1) * slots, :] = got[b][0:slots, :]
    whole = slots % 128 == 0
    if whole:
        keys = [jnp.concatenate(keys, 1)]
    span = lane_count if whole else slots
    for zone_at in range(zone_count):
        total = count = None
        for b, key in enumerate(keys):
            picker = hot(iota((lists_here, span), 0) + zone_at * lists_here == key)
            part = jnp.dot(
                picker.astype(BF16), rows[b * span : (b + 1) * span, :], preferred_element_type=F32
            )
            total = part if total is None else total + part
            if first:
                part = jnp.sum(picker, axis=1, keepdims=True)
                count = part if count is None else count + part
        if zone_at == 0:
            blocks[0][...] = total
        else:
            blocks[zone_at][0:lists_here, :] = total.astype(BF16)
        if first:
            eye = iota((lists_here, lists_here), 0) == iota((lists_here, lists_here), 1)
            line = jnp.sum(jnp.where(eye, count, 0.0), axis=0, keepdims=True)
            if zone_at == 0:
                count_ref[...] = jnp.where(iota(count_ref.shape, 0) == 2, over, line)
            else:
                number = line.astype(jnp.int32)
                high = (number >> 8).astype(F32)
                low = (number & 255).astype(F32)
                shape = (16, lists_here)
                extra = jnp.where(
                    iota(shape, 0) == 0, high, jnp.where(iota(shape, 0) == 1, low, over)
                )
                if width > lists_here:
                    extra = jnp.concatenate([extra, jnp.zeros((16, width - lists_here), F32)], 1)
                blocks[zone_at][lists_here:, :] = extra.astype(BF16)


def close_kernel(lists_here, width, chunks, zone_count, *refs):
    fill_ref, own_count = refs[:2]
    refs = refs[2:]
    drift_ref, count_ref, new_ref = refs[chunks * zone_count :]
    line = own_count[0:1, :]
    for at in range(1, zone_count):
        extra = refs[at][lists_here : lists_here + 16, 0:lists_here].astype(F32)
        line = line + extra[0:1, :] * 256.0 + extra[1:2, :]
    number = line.astype(jnp.int32)
    fill = fill_ref[...]
    count_ref[...] = number
    new_ref[...] = ((fill + number + 127) >> 7) - ((fill + 127) >> 7)
    eye = iota((lists_here, lists_here), 0) == iota((lists_here, lists_here), 1)
    divisor = jnp.sum(jnp.where(eye, jnp.maximum(line, 1.0), 0.0), axis=1, keepdims=True)
    for chunk in range(chunks):
        mine = refs[chunk * zone_count : (chunk + 1) * zone_count]
        total = mine[0][...]
        for at in range(1, zone_count):
            total = total + mine[at][0:lists_here, :].astype(F32)
        drift_ref[:, chunk * width : (chunk + 1) * width] = total / divisor


def decode_rows(codes, codebook):
    vec_rows, sub_count = codes.shape
    cent_count, feat_width = codebook.shape
    sub_width = feat_width // sub_count
    code_table = codebook.reshape(cent_count, sub_count, sub_width)
    block_rows = 256
    code_blocks = codes.reshape(vec_rows // block_rows, block_rows, sub_count)

    def one_block(code_block):
        picker = (
            code_block[:, :, None] == jnp.arange(cent_count, dtype=jnp.int32)[None, None, :]
        ).astype(jnp.bfloat16)
        picked = jnp.einsum("bmk,kmj->bmj", picker, code_table, preferred_element_type=jnp.float32)
        return picked.reshape(block_rows, feat_width)

    return lax.map(one_block, code_blocks).reshape(vec_rows, feat_width)


def sum_by_list(rows_in, tags_in, list_total):
    picker = (tags_in[:, None] == jnp.arange(list_total, dtype=jnp.int32)[None, :]).astype(
        jnp.bfloat16
    )
    list_sums = lax.dot_general(
        picker, rows_in, (((0,), (0,)), ((), ())), preferred_element_type=jnp.float32
    )
    counts = jnp.sum(picker, axis=0, dtype=jnp.float32)
    return (list_sums, counts)


def rank_in_block(owner_block, owner_total):
    vec_rows = owner_block.shape[0]
    picker = (owner_block[:, None] == jnp.arange(owner_total, dtype=jnp.int32)[None, :]).astype(
        jnp.bfloat16
    )
    later = (
        jnp.arange(vec_rows, dtype=jnp.int32)[:, None]
        > jnp.arange(vec_rows, dtype=jnp.int32)[None, :]
    )
    before = jnp.dot(later.astype(jnp.bfloat16), picker, preferred_element_type=jnp.float32)
    return jnp.sum(before * picker.astype(jnp.float32), axis=1).astype(jnp.int32)


def spread_all(residuals, codes, list_ids, rotation, codebook, list_fill):
    row_count = lax.axis_size("row")
    col_count = lax.axis_size("col")
    owner_total = row_count * col_count
    vec_rows, feat_width = residuals.shape
    lists_here = list_fill.shape[0]
    slot_cap = 3 * vec_rows // owner_total
    rotated = jnp.dot(residuals, rotation, preferred_element_type=jnp.float32)
    rebuilt = decode_rows(codes, codebook)
    encode_error = (rotated - rebuilt).astype(jnp.bfloat16)
    owner_block = list_ids // lists_here
    slot_index = owner_block * slot_cap + rank_in_block(owner_block, owner_total)
    send_rows = (
        jnp.zeros((owner_total * slot_cap, feat_width), jnp.bfloat16)
        .at[slot_index]
        .set(encode_error)
    )
    send_tags = jnp.full((owner_total * slot_cap,), -1, jnp.int32).at[slot_index].set(list_ids)
    send_rows = send_rows.reshape(row_count, col_count, slot_cap, feat_width)
    send_tags = send_tags.reshape(row_count, col_count, slot_cap)
    got_rows, got_tags = (
        lax.all_to_all(
            lax.all_to_all(send_rows, "row", split_axis=0, concat_axis=0, tiled=True),
            "col",
            split_axis=1,
            concat_axis=1,
            tiled=True,
        ),
        lax.all_to_all(
            lax.all_to_all(send_tags, "row", split_axis=0, concat_axis=0, tiled=True),
            "col",
            split_axis=1,
            concat_axis=1,
            tiled=True,
        ),
    )
    got_rows = got_rows.reshape(-1, feat_width)
    got_tags = got_tags.reshape(-1)
    list_base = (lax.axis_index("row") * col_count + lax.axis_index("col")) * lists_here
    local_index = jnp.where(got_tags >= 0, got_tags - list_base, -1)
    list_sums, counts = sum_by_list(got_rows, local_index, lists_here)
    list_counts = counts.astype(jnp.int32)
    divisor = jnp.maximum(list_counts, 1).astype(jnp.float32)
    list_drift = list_sums / divisor[:, None]
    new_blocks = (list_fill + list_counts + 127) // 128 - (list_fill + 127) // 128
    return (list_drift, list_counts, new_blocks)


def vmem(count):
    return [pl.BlockSpec(memory_space=pltpu.VMEM)] * count


def call(kernel, outs, scratch, ins, flops, specs=None):
    size = sum(a.size * a.dtype.itemsize for a in (*ins, *outs))
    return pl.pallas_call(
        kernel,
        out_shape=outs,
        in_specs=specs or vmem(len(ins)),
        out_specs=vmem(len(outs)),
        scratch_shapes=scratch,
        grid=() if specs is None else (1,),
        cost_estimate=pl.CostEstimate(flops=flops, bytes_accessed=size, transcendentals=0),
        compiler_params=pltpu.CompilerParams(vmem_limit_bytes=56 * 1024 * 1024),
    )(*ins)


def shape(dims, kind):
    return jax.ShapeDtypeStruct(dims, kind)


def local(residuals, codes, list_ids, rotation, codebook, list_fill):
    row_count = lax.axis_size("row")
    col_count = lax.axis_size("col")
    vecs, feats = residuals.shape
    subs = codes.shape[1]
    dsub = feats // subs
    cents = codebook.shape[0]
    lists_here = list_fill.shape[0]
    zone_count = col_count // 2
    width = split(feats, CHUNKS)
    chunks = feats // width
    bound = 3 * vecs // row_count
    slots = up(bound // 2, 16)

    def trade(array, axis, size, mask):
        return lax.ppermute(array, axis, [(i, i ^ mask) for i in range(size)])

    ids = list_ids.reshape(1, vecs)
    fill = list_fill.reshape(1, lists_here)
    extra = tag_rows(slots, width)
    packed = []
    slot = None
    for chunk in range(chunks):
        first = chunk == 0
        outs = [shape((slots + (extra if first else 0), width), BF16) for _ in range(row_count)]
        scratch = [
            pltpu.VMEM((width, vecs), F32),
            pltpu.VMEM((width, cents), F32),
            pltpu.VMEM((width, vecs), BF16),
        ]
        if first:
            outs += [shape((8, vecs), jnp.int32)]
        ins = (ids if first else slot, codes.T, residuals, rotation, codebook)

        def all_of(array):
            return pl.BlockSpec(array.shape, lambda i: (0, 0))

        def columns(array, chunk=chunk):
            return pl.BlockSpec((array.shape[0], width), lambda i: (0, chunk))

        specs = [*map(all_of, ins[:3]), columns(rotation), columns(codebook)]
        got = call(
            functools.partial(
                pack_kernel, first, slots, chunk * width, width, dsub, lists_here, row_count, col_count
            ),
            outs,
            scratch,
            ins,
            2 * vecs * width * (feats + row_count * slots),
            specs,
        )
        packed.append(got[:row_count])
        if first:
            slot = got[row_count]
    blocks = []
    key = count = None
    for chunk in range(chunks):
        first = chunk == 0
        mine = packed[chunk]
        got = [mine[0]] + [None] * (row_count - 1)
        for mask in sorted(range(1, row_count), key=lambda m: -bin(m).count("1")):
            got[mask] = trade(mine[mask], "row", row_count, mask)
        other = [trade(got[0], "col", col_count, 1)]
        other += [trade(array, "col", col_count, 1) for array in got[1:]]
        outs = [shape((lists_here, width), F32)]
        outs += [
            shape((lists_here + (16 if first else 0), width), BF16) for _ in range(zone_count - 1)
        ]
        ins = [*got, *other]
        if first:
            outs += [shape((8, lists_here), F32), shape((2 * row_count, slots), jnp.int32)]
        else:
            ins = [key, *ins]
        sums = call(
            functools.partial(sum_kernel, first, slots, width, lists_here, row_count, zone_count),
            outs,
            [pltpu.VMEM((2 * row_count * slots, width), BF16)],
            ins,
            2 * zone_count * lists_here * 2 * row_count * slots * width,
        )
        if first:
            count, key = sums[zone_count:]
        blocks.append(sums[:zone_count])
    landed = []
    for chunk in range(chunks):
        mine = blocks[chunk]
        landed.append(mine[0])
        got = [None] * zone_count
        for mask in sorted(range(1, zone_count), key=lambda m: -m):
            got[mask] = trade(mine[mask], "col", col_count, 2 * mask)
        landed += got[1:]
    over = count[2, 0]
    for array in landed[1:zone_count]:
        over = over + array[lists_here + 2, 0].astype(F32)

    def close(*arrays):
        drift, counts, new_blocks = call(
            functools.partial(close_kernel, lists_here, width, chunks, zone_count),
            [
                shape((lists_here, feats), F32),
                shape((1, lists_here), jnp.int32),
                shape((1, lists_here), jnp.int32),
            ],
            [],
            [fill, count, *arrays],
            lists_here * feats * zone_count,
        )
        return drift, counts.reshape(-1), new_blocks.reshape(-1)

    return lax.cond(
        over > 0,
        lambda *arrays: spread_all(residuals, codes, list_ids, rotation, codebook, list_fill),
        close,
        *landed,
    )


def solution(mesh):
    placed = (
        P(("row", "col"), None),
        P(("row", "col"), None),
        P(("row", "col")),
        P(),
        P(),
        P(("row", "col")),
    )
    return jax.shard_map(
        local,
        mesh=mesh,
        in_specs=placed,
        out_specs=(P(("row", "col"), None), P(("row", "col")), P(("row", "col"))),
        check_vma=False,
    )
```

```python
import functools

import jax
import jax.numpy as jnp
from jax import lax
from jax.experimental import pallas as pl
from jax.experimental.pallas import tpu as pltpu
from jax.sharding import PartitionSpec as P


CUT = (2, 2, 2)
F32 = jnp.float32
BF16 = jnp.bfloat16
NT = (((1,), (1,)), ((), ()))


def up(value, step):
    return (value + step - 1) // step * step


def tag_rows(slots, width):
    return up(8 * (-(-slots // width)), 16)


def iota(shape, dim):
    return lax.broadcasted_iota(jnp.int32, shape, dim)


def hot(test):
    return jnp.where(test, 1.0, 0.0).astype(F32)


def plan_slots(ids, slots, lists_here, row_count, col_count):
    me = lax.axis_index("row")
    vecs = ids.shape[1]
    owner = ids // lists_here
    group = (owner // col_count) ^ me
    owner_col = owner % col_count
    in_list = ids % lists_here
    sub = max(8, row_count)
    member = hot(iota((sub, vecs), 0) == group)
    run = member
    lane = iota((sub, vecs), 1)
    step = 1
    while step < vecs:
        run = run + jnp.where(lane >= step, pltpu.roll(run, step, 1), 0.0)
        step *= 2
    over = jnp.max(hot(run > float(slots)), axis=1, keepdims=True)
    over = jnp.max(over, axis=0, keepdims=True)
    rank = jnp.sum((run - member) * member, axis=0, keepdims=True).astype(jnp.int32)
    slot = jnp.where(rank < slots, group * slots + rank, -1)
    tags = jnp.where(
        iota((16, vecs), 0) == 0,
        (owner_col + 1).astype(F32),
        jnp.where(iota((16, vecs), 0) == 1, in_list.astype(F32), 0.0),
    )
    return slot, tags.astype(BF16), over


def pack_kernel(first, slots, base, width, dsub, lists_here, row_count, col_count, *refs):
    if first:
        ids_ref, ct_ref, res_ref, rot_ref, book_ref = refs[:5]
        outs = refs[5 : 5 + row_count]
        slot_ref, rot_t, tab_t, err_t = refs[5 + row_count :]
        slot, tags, over = plan_slots(ids_ref[...], slots, lists_here, row_count, col_count)
        slot_ref[...] = jnp.broadcast_to(slot, slot_ref.shape)
    else:
        slot_ref, ct_ref, res_ref, rot_ref, book_ref = refs[:5]
        outs = refs[5 : 5 + row_count]
        rot_t, tab_t, err_t = refs[5 + row_count :]
        slot = slot_ref[0:1, :]
    vecs = res_ref.shape[0]
    cents = book_ref.shape[0]
    here = slice(base, base + width)
    tab_t[...] = book_ref[:, here].astype(F32).T
    rot_t[...] = lax.dot_general(
        rot_ref[:, here], res_ref[...], (((0,), (1,)), ((), ())), preferred_element_type=F32
    )

    for block in range(vecs // 128):
        here = slice(block * 128, (block + 1) * 128)

        def half(row):
            first_sub = (base + row) // dsub
            last_sub = (base + row + 7) // dsub
            index = jnp.broadcast_to(ct_ref[first_sub : first_sub + 1, here], (8, 128))
            for sub in range(first_sub + 1, last_sub + 1):
                starts = sub * dsub - (base + row)
                other = jnp.broadcast_to(ct_ref[sub : sub + 1, here], (8, 128))
                index = jnp.where(iota((8, 128), 0) >= starts, other, index)
            low = index & 127
            value = None
            for part in range(0, cents, 128):
                got = jnp.take_along_axis(
                    tab_t[row : row + 8, part : part + 128], low, axis=1, mode="promise_in_bounds"
                )
                value = got if value is None else jnp.where(index >= part, got, value)
            return rot_t[row : row + 8, here] - value

        for row in range(0, width, 16):
            err_t[row : row + 16, here] = jnp.concatenate([half(row), half(row + 8)], 0).astype(BF16)

    picker = hot(iota((row_count * slots, vecs), 0) == slot).astype(BF16)
    rows = lax.dot_general(picker, err_t[...], NT, preferred_element_type=F32).astype(BF16)
    for group in range(row_count):
        outs[group][0:slots, :] = rows[group * slots : (group + 1) * slots, :]
    if not first:
        return
    lines = lax.dot_general(tags, picker, NT, preferred_element_type=F32)[0:8, :]
    lines = jnp.where(iota(lines.shape, 0) == 2, over, lines)
    for group in range(row_count):
        line = lines[:, group * slots : (group + 1) * slots]
        extra = outs[group].shape[0] - slots
        parts = [line[:, at : min(at + width, slots)] for at in range(0, slots, width)]
        parts = [
            part
            if part.shape[1] == width
            else jnp.concatenate([part, jnp.zeros((8, width - part.shape[1]), F32)], 1)
            for part in parts
        ]
        while len(parts) * 8 < extra:
            parts.append(jnp.zeros((8, width), F32))
        outs[group][slots:, :] = jnp.concatenate(parts, 0).astype(BF16)


def sum_kernel(first, slots, width, lists_here, row_count, zone_count, *refs):
    senders = 2 * row_count
    refs = list(refs)
    key_in = None if first else refs.pop(0)
    got, refs = refs[:senders], refs[senders:]
    own, send = refs[:2]
    rows = refs.pop()
    kept = refs[2:3] if zone_count > 2 else []
    over = None
    if first:
        count_ref, key_ref = refs[-2:]
        me = lax.axis_index("col")
        zone, core = me // 2, me % 2
        keys = []
        over = jnp.zeros((1, 1), F32)
        for ref in got:
            extra = ref[slots:, :].astype(F32)
            pieces = -(-slots // width)
            over = over + extra[2:3, 0:1]
            line = jnp.concatenate([extra[8 * p : 8 * p + 8, :] for p in range(pieces)], 1)
            line = line[:, 0:slots].astype(jnp.int32)
            owner_col = line[0:1, :] - 1
            key = ((owner_col >> 1) ^ zone) * lists_here + line[1:2, :]
            mine = (owner_col >= 0) & ((owner_col & 1) == core)
            keys.append(jnp.where(mine, key, -1))
        for b in range(senders):
            key_ref[b : b + 1, :] = keys[b]
    else:
        keys = [key_in[b : b + 1, :] for b in range(senders)]
    for b in range(senders):
        rows[b * slots : (b + 1) * slots, :] = got[b][0:slots, :]
    whole = slots % 128 == 0
    if whole:
        keys = [jnp.concatenate(keys, 1)]
    span = senders * slots if whole else slots
    counts = []
    for at in range(zone_count):
        total = count = None
        for b, key in enumerate(keys):
            picker = hot(iota((lists_here, span), 0) + at * lists_here == key)
            part = jnp.dot(
                picker.astype(BF16), rows[b * span : (b + 1) * span, :], preferred_element_type=F32
            )
            total = part if total is None else total + part
            if first:
                part = jnp.sum(picker, axis=1, keepdims=True)
                count = part if count is None else count + part
        line = None
        if first:
            eye = iota((lists_here, lists_here), 0) == iota((lists_here, lists_here), 1)
            line = jnp.sum(jnp.where(eye, count, 0.0), axis=0, keepdims=True)
        if at % 2:
            put_block(send, at // 2, lists_here, total, line, over)
        else:
            if at == 0:
                own[...] = total
            else:
                kept[0][(at // 2 - 1) * lists_here : at // 2 * lists_here, :] = total
            counts.append(line)
    if first:
        put_counts(count_ref, counts, over)


def put_block(send, place, lists_here, total, line, over):
    rows = lists_here + (0 if line is None else 16)
    width = total.shape[1]
    send[place * rows : place * rows + lists_here, :] = total.astype(BF16)
    if line is None:
        return
    number = line.astype(jnp.int32)
    high = (number >> 8).astype(F32)
    low = (number & 255).astype(F32)
    kind = iota((16, lists_here), 0)
    extra = jnp.where(kind == 0, high, jnp.where(kind == 1, low, over))
    if width > lists_here:
        extra = jnp.concatenate([extra, jnp.zeros((16, width - lists_here), F32)], 1)
    send[place * rows + lists_here : (place + 1) * rows, :] = extra.astype(BF16)


def put_counts(count_ref, counts, over):
    kind = iota(count_ref.shape, 0)
    table = jnp.where(kind == count_ref.shape[0] - 1, over, 0.0)
    for place, line in enumerate(counts):
        table = jnp.where(kind == place, line, table)
    count_ref[...] = table


def get_counts(got, place, lists_here):
    rows = lists_here + 16
    extra = got[place * rows + lists_here : (place + 1) * rows, 0:lists_here].astype(F32)
    return extra[0:1, :] * 256.0 + extra[1:2, :], extra[2:3, 0:1]


def halve_kernel(first, lists_here, blocks, *refs):
    refs = list(refs)
    table = refs.pop(0) if first else None
    got, kept = refs[:2]
    send = refs[2]
    rest = refs[3:]
    rows = lists_here + (16 if first else 0)
    over = None
    counts = []
    for at in range(blocks):
        line = None
        if first:
            line, more = get_counts(got, at, lists_here)
            line = line + table[at : at + 1, :]
            over = more + table[table.shape[0] - 1 :, 0:1]
        if at > 0:
            total = kept[(at - 1) * lists_here : at * lists_here, :]
            total = total + got[at * rows : at * rows + lists_here, :].astype(F32)
            if at % 2:
                put_block(send, at // 2, lists_here, total, line, over)
            else:
                rest[0][(at // 2 - 1) * lists_here : at // 2 * lists_here, :] = total
        if at % 2 == 0:
            counts.append(line)
    if first:
        put_counts(rest[-1], counts, over)


def close_kernel(lists_here, widths, levels, *refs):
    fill_ref, table = refs[:2]
    refs = refs[2:]
    chunks = len(widths)
    drift_ref, count_ref, new_ref = refs[chunks * (1 + levels) :]
    line, _ = get_counts(refs[levels], 0, lists_here)
    line = line + table[0:1, :]
    number = line.astype(jnp.int32)
    fill = fill_ref[...]
    count_ref[...] = number
    new_ref[...] = ((fill + number + 127) >> 7) - ((fill + 127) >> 7)
    eye = iota((lists_here, lists_here), 0) == iota((lists_here, lists_here), 1)
    divisor = jnp.sum(jnp.where(eye, jnp.maximum(line, 1.0), 0.0), axis=1, keepdims=True)
    base = 0
    for chunk, width in enumerate(widths):
        own, *got = refs[chunk * (1 + levels) : (chunk + 1) * (1 + levels)]
        total = own[...]
        for array in got:
            total = total + array[0:lists_here, :].astype(F32)
        drift_ref[:, base : base + width] = total / divisor
        base += width


def decode_rows(codes, codebook):
    vec_rows, sub_count = codes.shape
    cent_count, feat_width = codebook.shape
    sub_width = feat_width // sub_count
    code_table = codebook.reshape(cent_count, sub_count, sub_width)
    block_rows = 256
    code_blocks = codes.reshape(vec_rows // block_rows, block_rows, sub_count)

    def one_block(code_block):
        picker = (
            code_block[:, :, None] == jnp.arange(cent_count, dtype=jnp.int32)[None, None, :]
        ).astype(jnp.bfloat16)
        picked = jnp.einsum("bmk,kmj->bmj", picker, code_table, preferred_element_type=jnp.float32)
        return picked.reshape(block_rows, feat_width)

    return lax.map(one_block, code_blocks).reshape(vec_rows, feat_width)


def sum_by_list(rows_in, tags_in, list_total):
    picker = (tags_in[:, None] == jnp.arange(list_total, dtype=jnp.int32)[None, :]).astype(
        jnp.bfloat16
    )
    list_sums = lax.dot_general(
        picker, rows_in, (((0,), (0,)), ((), ())), preferred_element_type=jnp.float32
    )
    counts = jnp.sum(picker, axis=0, dtype=jnp.float32)
    return (list_sums, counts)


def rank_in_block(owner_block, owner_total):
    vec_rows = owner_block.shape[0]
    picker = (owner_block[:, None] == jnp.arange(owner_total, dtype=jnp.int32)[None, :]).astype(
        jnp.bfloat16
    )
    later = (
        jnp.arange(vec_rows, dtype=jnp.int32)[:, None]
        > jnp.arange(vec_rows, dtype=jnp.int32)[None, :]
    )
    before = jnp.dot(later.astype(jnp.bfloat16), picker, preferred_element_type=jnp.float32)
    return jnp.sum(before * picker.astype(jnp.float32), axis=1).astype(jnp.int32)


def spread_all(residuals, codes, list_ids, rotation, codebook, list_fill):
    row_count = lax.axis_size("row")
    col_count = lax.axis_size("col")
    owner_total = row_count * col_count
    vec_rows, feat_width = residuals.shape
    lists_here = list_fill.shape[0]
    slot_cap = 3 * vec_rows // owner_total
    rotated = jnp.dot(residuals, rotation, preferred_element_type=jnp.float32)
    rebuilt = decode_rows(codes, codebook)
    encode_error = (rotated - rebuilt).astype(jnp.bfloat16)
    owner_block = list_ids // lists_here
    slot_index = owner_block * slot_cap + rank_in_block(owner_block, owner_total)
    send_rows = (
        jnp.zeros((owner_total * slot_cap, feat_width), jnp.bfloat16)
        .at[slot_index]
        .set(encode_error)
    )
    send_tags = jnp.full((owner_total * slot_cap,), -1, jnp.int32).at[slot_index].set(list_ids)
    send_rows = send_rows.reshape(row_count, col_count, slot_cap, feat_width)
    send_tags = send_tags.reshape(row_count, col_count, slot_cap)
    got_rows, got_tags = (
        lax.all_to_all(
            lax.all_to_all(send_rows, "row", split_axis=0, concat_axis=0, tiled=True),
            "col",
            split_axis=1,
            concat_axis=1,
            tiled=True,
        ),
        lax.all_to_all(
            lax.all_to_all(send_tags, "row", split_axis=0, concat_axis=0, tiled=True),
            "col",
            split_axis=1,
            concat_axis=1,
            tiled=True,
        ),
    )
    got_rows = got_rows.reshape(-1, feat_width)
    got_tags = got_tags.reshape(-1)
    list_base = (lax.axis_index("row") * col_count + lax.axis_index("col")) * lists_here
    local_index = jnp.where(got_tags >= 0, got_tags - list_base, -1)
    list_sums, counts = sum_by_list(got_rows, local_index, lists_here)
    list_counts = counts.astype(jnp.int32)
    divisor = jnp.maximum(list_counts, 1).astype(jnp.float32)
    list_drift = list_sums / divisor[:, None]
    new_blocks = (list_fill + list_counts + 127) // 128 - (list_fill + 127) // 128
    return (list_drift, list_counts, new_blocks)


def vmem(count):
    return [pl.BlockSpec(memory_space=pltpu.VMEM)] * count


def call(kernel, outs, scratch, ins, flops):
    size = sum(a.size * a.dtype.itemsize for a in (*ins, *outs))
    return pl.pallas_call(
        kernel,
        out_shape=outs,
        in_specs=vmem(len(ins)),
        out_specs=vmem(len(outs)),
        scratch_shapes=scratch,
        cost_estimate=pl.CostEstimate(flops=flops, bytes_accessed=size, transcendentals=0),
        compiler_params=pltpu.CompilerParams(vmem_limit_bytes=28 * 1024 * 1024),
    )(*ins)


def shape(dims, kind):
    return jax.ShapeDtypeStruct(dims, kind)


def cut(feats):
    units = feats // 128
    if feats % 128 or units < 3:
        return [feats]
    head, tail = CUT[0] * units // 6, CUT[2] * units // 6
    return [w * 128 for w in (head, units - head - tail, tail) if w]


def local(residuals, codes, list_ids, rotation, codebook, list_fill):
    row_count = lax.axis_size("row")
    col_count = lax.axis_size("col")
    vecs, feats = residuals.shape
    dsub = feats // codes.shape[1]
    cents = codebook.shape[0]
    lists_here = list_fill.shape[0]
    zone_count = col_count // 2
    widths = cut(feats)
    bound = 3 * vecs // row_count
    slots = up(bound // 2, 16)

    def trade(array, axis, size, mask):
        return lax.ppermute(array, axis, [(i, i ^ mask) for i in range(size)])

    ids = list_ids.reshape(1, vecs)
    fill = list_fill.reshape(1, lists_here)
    packed = []
    slot = None
    for chunk, width in enumerate(widths):
        first = chunk == 0
        extra = tag_rows(slots, width) if first else 0
        outs = [shape((slots + extra, width), BF16) for _ in range(row_count)]
        scratch = [
            pltpu.VMEM((width, vecs), F32),
            pltpu.VMEM((width, cents), F32),
            pltpu.VMEM((width, vecs), BF16),
        ]
        if first:
            outs += [shape((8, vecs), jnp.int32)]
        ins = (ids if first else slot, codes.T, residuals, rotation, codebook)
        base = sum(widths[:chunk])
        got = call(
            functools.partial(
                pack_kernel, first, slots, base, width, dsub, lists_here, row_count, col_count
            ),
            outs,
            scratch,
            ins,
            2 * vecs * width * (feats + row_count * slots),
        )
        packed.append(got[:row_count])
        if first:
            slot = got[row_count]
    own = []
    moved = []
    key = table = None
    for chunk, width in enumerate(widths):
        first = chunk == 0
        extra = 16 if first else 0
        mine = packed[chunk]
        got = [mine[0]] + [None] * (row_count - 1)
        for mask in sorted(range(1, row_count), key=lambda m: -bin(m).count("1")):
            got[mask] = trade(mine[mask], "row", row_count, mask)
        other = [trade(got[0], "col", col_count, 1)]
        other += [trade(array, "col", col_count, 1) for array in got[1:]]
        blocks = zone_count // 2
        outs = [
            shape((lists_here, width), F32),
            shape((blocks * (lists_here + extra), width), BF16),
        ]
        if blocks > 1:
            outs += [shape(((blocks - 1) * lists_here, width), F32)]
        ins = [*got, *other]
        if first:
            outs += [shape((16, lists_here), F32), shape((2 * row_count, slots), jnp.int32)]
        else:
            ins = [key, *ins]
        sums = call(
            functools.partial(sum_kernel, first, slots, width, lists_here, row_count, zone_count),
            outs,
            [pltpu.VMEM((2 * row_count * slots, width), BF16)],
            ins,
            2 * zone_count * lists_here * 2 * row_count * slots * width,
        )
        if first:
            table, key = sums[-2:]
        own.append(sums[0])
        moved.append(sums[1 : 3 if blocks > 1 else 2])
    landed = []
    levels = 0
    for chunk, width in enumerate(widths):
        first = chunk == 0
        extra = 16 if first else 0
        send, *kept = moved[chunk]
        landed.append(own[chunk])
        levels = 0
        blocks = zone_count // 2
        while blocks:
            got = trade(send, "col", col_count, 2 << levels)
            landed.append(got)
            levels += 1
            half = blocks // 2
            if half:
                outs = [shape((half * (lists_here + extra), width), BF16)]
                if half > 1:
                    outs += [shape(((half - 1) * lists_here, width), F32)]
                if first:
                    outs += [shape((16, lists_here), F32)]
                send, *kept = call(
                    functools.partial(halve_kernel, first, lists_here, blocks),
                    outs,
                    [],
                    [*([table] if first else []), got, *kept],
                    blocks * lists_here * width,
                )
                if first:
                    table = kept.pop()
            blocks = half
    over = table[15, 0] + landed[levels][lists_here + 2, 0].astype(F32)

    def close(*arrays):
        drift, counts, new_blocks = call(
            functools.partial(close_kernel, lists_here, widths, levels),
            [
                shape((lists_here, feats), F32),
                shape((1, lists_here), jnp.int32),
                shape((1, lists_here), jnp.int32),
            ],
            [],
            [fill, table, *arrays],
            lists_here * feats * zone_count,
        )
        return drift, counts.reshape(-1), new_blocks.reshape(-1)

    return lax.cond(
        over > 0,
        lambda *arrays: spread_all(residuals, codes, list_ids, rotation, codebook, list_fill),
        close,
        *landed,
    )


def solution(mesh):
    placed = (
        P(("row", "col"), None),
        P(("row", "col"), None),
        P(("row", "col")),
        P(),
        P(),
        P(("row", "col")),
    )
    return jax.shard_map(
        local,
        mesh=mesh,
        in_specs=placed,
        out_specs=(P(("row", "col"), None), P(("row", "col")), P(("row", "col"))),
        check_vma=False,
    )
```
